32 devices in a mesh: shard: 4 (over z), ctx: 2 (over y), tp: 4 (over x, core).
Axes of the slice: x: 2, y: 2, z: 4, core: 2. Of those that a mesh axis runs over, the one named last changes fastest.
Arguments:
- inputs: bfloat16 [4, 2048, 1536], P('shard', 'ctx'), may hold values from -6 to 6
- text_states: bfloat16 [64, 1536], replicated, may hold values from -6 to 6
- query_self: bfloat16 [1536, 1536], P('shard', 'tp'), may hold values from -0.15625 to 0.15625
- key_self: bfloat16 [1536, 1536], P('shard', 'tp'), may hold values from -0.15625 to 0.15625
- value_self: bfloat16 [1536, 1536], P('shard', 'tp'), may hold values from -0.15625 to 0.15625
- output_self: bfloat16 [1536, 1536], P('tp', 'shard'), may hold values from -2.5 to 2.5
- query_cross: bfloat16 [1536, 1536], P('shard', 'tp'), may hold values from -0.15625 to 0.15625
- key_cross: bfloat16 [1536, 1536], P('shard', 'tp'), may hold values from -0.15625 to 0.15625
- value_cross: bfloat16 [1536, 1536], P('shard', 'tp'), may hold values from -0.15625 to 0.15625
- output_cross: bfloat16 [1536, 1536], P('tp', 'shard'), may hold values from -0.875 to 0.875
- up_weight: bfloat16 [1536, 6144], P('shard', 'tp'), may hold values from -0.15625 to 0.15625
- down_weight: bfloat16 [6144, 1536], P('tp', 'shard'), may hold values from -0.078125 to 0.078125
- gain_self: bfloat16 [1536], P('shard'), may hold values from 0.5 to 1.5
- bias_self: bfloat16 [1536], P('shard'), may hold values from -3 to 3
- gain_cross: bfloat16 [1536], P('shard'), may hold values from 0.5 to 1.5
- bias_cross: bfloat16 [1536], P('shard'), may hold values from -3 to 3
- gain_feed: bfloat16 [1536], P('shard'), may hold values from 0.5 to 1.5
- bias_feed: bfloat16 [1536], P('shard'), may hold values from -3 to 3
- cotangent: bfloat16 [4, 2048, 1536], P('shard', 'ctx'), may hold values from -6 to 6
Outputs:
- layer_out: bfloat16 [4, 2048, 1536], P('shard', 'ctx')
- input_grad: bfloat16 [4, 2048, 1536], P('shard', 'ctx')
- text_grad: float32 [64, 1536], replicated
- queryself_grad: float32 [1536, 1536], P('shard', 'tp')
- keyself_grad: float32 [1536, 1536], P('shard', 'tp')
- valueself_grad: float32 [1536, 1536], P('shard', 'tp')
- outputself_grad: float32 [1536, 1536], P('tp', 'shard')
- querycross_grad: float32 [1536, 1536], P('shard', 'tp')
- keycross_grad: float32 [1536, 1536], P('shard', 'tp')
- valuecross_grad: float32 [1536, 1536], P('shard', 'tp')
- outputcross_grad: float32 [1536, 1536], P('tp', 'shard')
- up_grad: float32 [1536, 6144], P('shard', 'tp')
- down_grad: float32 [6144, 1536], P('tp', 'shard')
- gainself_grad: float32 [1536], P('shard')
- biasself_grad: float32 [1536], P('shard')
- gaincross_grad: float32 [1536], P('shard')
- biascross_grad: float32 [1536], P('shard')
- gainfeed_grad: float32 [1536], P('shard')
- biasfeed_grad: float32 [1536], P('shard')
The draws below stay inside these ranges and needn't reach their ends.
All inputs are finite; a program needn't handle non-finite values.
Results may differ from the reference program's by a relative error of at most 0.015.
Values may be sent and summed in bfloat16 or wider, within the bound.
A program may use at most 192 MiB of HBM per device.

```python
import jax
import jax.numpy as jnp
from jax import lax

D = 1536
HEADS = 24
HEAD_DIM = 64
FF = 6144
TEXT = 64
HD = 1536
FRAMES = 2048
CLIPS = 4


def block_levels(rng, shape, cuts, least, largest):
    def one(dim, parts):
        steps = jax.random.uniform(jax.random.fold_in(jax.random.fold_in(rng, 6), dim), (parts,), jnp.float32, least / len(cuts), largest / len(cuts))
        return jnp.repeat(jnp.exp(steps), shape[dim] // parts).reshape((-1,) + (1,) * (len(shape) - dim - 1))

    factor_of = one(*cuts[0])
    for cut in cuts[1:]:
        factor_of = factor_of * one(*cut)
    return factor_of


def centred(key, dims, spread, bound, cuts=(), held_as=jnp.bfloat16):
    drawn = spread * jax.random.normal(key, dims, jnp.float32)
    if cuts:
        drawn = drawn * block_levels(key, dims, cuts, -0.22, 0.18)
    return jnp.clip(drawn, -bound, bound).astype(held_as)


def setup_inputs(seed: int = 0) -> dict:
    keys = jax.random.split(jax.random.key(seed), 20)
    inputs = centred(keys[0], (CLIPS, FRAMES, D), 1.0, 6.0, ((0, 4), (1, 2)))
    text_states = centred(keys[1], (TEXT, D), 1.0, 6.0)
    query_self = centred(keys[2], (D, HD), D ** -0.5, 0.15625, ((0, 4), (1, 4)))
    key_self = centred(keys[3], (D, HD), D ** -0.5, 0.15625, ((0, 4), (1, 4)))
    value_self = centred(keys[4], (D, HD), D ** -0.5, 0.15625, ((0, 4), (1, 4)))
    output_self = centred(keys[5], (HD, D), (max(HD * 8 // FRAMES, 4)) ** -0.5, 2.5, ((0, 4), (1, 4)))
    query_cross = centred(keys[6], (D, HD), D ** -0.5, 0.15625, ((0, 4), (1, 4)))
    key_cross = centred(keys[7], (D, HD), D ** -0.5, 0.15625, ((0, 4), (1, 4)))
    value_cross = centred(keys[8], (D, HD), D ** -0.5, 0.15625, ((0, 4), (1, 4)))
    output_cross = centred(keys[9], (HD, D), (max(HD // 32, 2)) ** -0.5, 0.875, ((0, 4), (1, 4)))
    up_weight = centred(keys[10], (D, FF), D ** -0.5, 0.15625, ((0, 4), (1, 4)))
    down_weight = centred(keys[11], (FF, D), FF ** -0.5, 0.078125, ((0, 4), (1, 4)))
    gain_self = jnp.clip(1.0 + 0.1 * jax.random.normal(keys[12], (D,), jnp.float32), 0.5, 1.5).astype(jnp.bfloat16)
    bias_self = centred(keys[13], (D,), 0.5, 3.0, ((0, 4),))
    gain_cross = jnp.clip(1.0 + 0.1 * jax.random.normal(keys[14], (D,), jnp.float32), 0.5, 1.5).astype(jnp.bfloat16)
    bias_cross = centred(keys[15], (D,), 0.5, 3.0, ((0, 4),))
    gain_feed = jnp.clip(1.0 + 0.1 * jax.random.normal(keys[16], (D,), jnp.float32), 0.5, 1.5).astype(jnp.bfloat16)
    bias_feed = centred(keys[17], (D,), 0.5, 3.0, ((0, 4),))
    cotangent = centred(keys[18], (CLIPS, FRAMES, D), 1.0, 6.0, ((0, 4), (1, 2)))
    return {"inputs": inputs, "text_states": text_states, "query_self": query_self, "key_self": key_self, "value_self": value_self, "output_self": output_self, "query_cross": query_cross, "key_cross": key_cross, "value_cross": value_cross, "output_cross": output_cross, "up_weight": up_weight, "down_weight": down_weight, "gain_self": gain_self, "bias_self": bias_self, "gain_cross": gain_cross, "bias_cross": bias_cross, "gain_feed": gain_feed, "bias_feed": bias_feed, "cotangent": cotangent}


@jax.custom_vjp
def low(v):
    return lax.optimization_barrier(v.astype(jnp.bfloat16)).astype(jnp.float32)

@jax.custom_vjp
def low_back(v):
    return v

def low_keep(v):
    return (low(v), None)

def low_pass(kept, grad):
    return (grad,)

def back_keep(v):
    return (v, None)

def back_low(kept, grad):
    return (low(grad),)
low.defvjp(low_keep, low_pass)
low_back.defvjp(back_keep, back_low)
EPSILON = 1e-05
HIGH = lax.Precision.HIGHEST

def layer_norm(values, gain_vec, bias_vec):
    centered = values - lax.optimization_barrier(jnp.mean(values, axis=-1, keepdims=True))
    variance = lax.optimization_barrier(jnp.mean(centered * centered, axis=-1, keepdims=True))
    return centered * lax.rsqrt(variance + EPSILON) * gain_vec + bias_vec

def matmul(left, right):
    return jnp.dot(left, right, precision=HIGH)

def split_heads(values):
    return values.reshape(values.shape[0], HEADS, HEAD_DIM)

def attention(queries, key_rows, value_rows, allowed):
    scaling = HEAD_DIM ** (-0.5)
    scores = low_back(jnp.einsum('qhd,khd->hqk', queries, key_rows, precision=HIGH) * scaling)
    scores = jnp.where(allowed[None], scores, -1e+30)
    attn_prob = jax.nn.softmax(scores, axis=-1)
    mixed = jnp.einsum('hqk,khd->qhd', low(attn_prob), value_rows, precision=HIGH)
    return low_back(low(mixed)).reshape(queries.shape[0], HEADS * HEAD_DIM)

def forward(inputs, text_states, query_self, key_self, value_self, output_self, query_cross, key_cross, value_cross, output_cross, up_weight, down_weight, gain_self, bias_self, gain_cross, bias_cross, gain_feed, bias_feed):
    key_text = split_heads(low(matmul(text_states, key_cross)))
    value_text = split_heads(low(matmul(text_states, value_cross)))
    position = jnp.arange(FRAMES)
    causal = position[:, None] >= position[None, :]
    open_mask = jnp.ones((FRAMES, TEXT), dtype=bool)

    def one_clip(stream):
        normed = low(layer_norm(stream, gain_self, bias_self))
        queries = split_heads(low_back(low(matmul(normed, query_self))))
        key_rows = split_heads(low_back(low(matmul(normed, key_self))))
        value_rows = split_heads(low_back(low(matmul(normed, value_self))))
        attended = attention(queries, key_rows, value_rows, causal)
        after_self = stream + low_back(matmul(attended, output_self))
        normed_cross = low(layer_norm(after_self, gain_cross, bias_cross))
        cross_rows = split_heads(low_back(low(matmul(normed_cross, query_cross))))
        crossed = attention(cross_rows, key_text, value_text, open_mask)
        after_cross = after_self + low_back(matmul(crossed, output_cross))
        normed_feed = low(layer_norm(after_cross, gain_feed, bias_feed))
        hidden = low(jax.nn.gelu(low_back(matmul(normed_feed, up_weight)), approximate=False))
        return after_cross + low_back(matmul(hidden, down_weight))
    return lax.map(jax.checkpoint(one_clip), inputs)

def reference(inputs, text_states, query_self, key_self, value_self, output_self, query_cross, key_cross, value_cross, output_cross, up_weight, down_weight, gain_self, bias_self, gain_cross, bias_cross, gain_feed, bias_feed, cotangent):
    floats = tuple((array_in.astype(jnp.float32) for array_in in (inputs, text_states, query_self, key_self, value_self, output_self, query_cross, key_cross, value_cross, output_cross, up_weight, down_weight, gain_self, bias_self, gain_cross, bias_cross, gain_feed, bias_feed)))
    result, pullback = jax.vjp(forward, *floats)
    grads = pullback(cotangent.astype(jnp.float32))
    return (result.astype(jnp.bfloat16), grads[0].astype(jnp.bfloat16), grads[1], grads[2], grads[3], grads[4], grads[5], grads[6], grads[7], grads[8], grads[9], grads[10], grads[11], grads[12], grads[13], grads[14], grads[15], grads[16], grads[17])
```

```python
import functools

import jax
import jax.numpy as jnp
from jax import lax
from jax.experimental import pallas as pl
from jax.experimental.pallas import tpu as pltpu
from jax.sharding import PartitionSpec as P

HEAD_DIM = 64
SCALING = HEAD_DIM ** (-0.5)
EPSILON = 1e-05
HIGH = lax.Precision.HIGHEST
F32 = jnp.float32
BF16 = jnp.bfloat16
TILE = 256
LANES = 128
CHUNKS = 2

NT = (((1,), (1,)), ((), ()))
NN = (((1,), (0,)), ((), ()))
TN = (((0,), (0,)), ((), ()))


def dot(left, right, dims=NN):
    return lax.dot_general(left, right, dims, preferred_element_type=F32)


def head_lanes(head, shape):
    lane = lax.broadcasted_iota(jnp.int32, shape, 1)
    return (lane >= head * HEAD_DIM) & (lane < head * HEAD_DIM + HEAD_DIM)


def attend_kernel(chunk, flag_ref, q_ref, kl_ref, vl_ref, kr_ref, vr_ref, out_ref, lse_ref):
    head = pl.program_id(0) % 2
    rows = q_ref.shape[0]

    def run(remote):
        for t in range(rows // TILE):
            here = pl.ds(t * TILE, TILE)
            mask = head_lanes(head, (TILE, LANES))
            query = jnp.where(mask, q_ref[here, :] * BF16(SCALING), BF16(0))
            full = chunk * rows + t * TILE
            parts = []
            if remote:
                parts.append((dot(query, kr_ref[...], NT), vr_ref[...]))
            if full:
                parts.append((dot(query, kl_ref[pl.ds(0, full), :], NT), vl_ref[pl.ds(0, full), :]))
            scores = dot(query, kl_ref[pl.ds(full, TILE), :], NT)
            keep = lax.broadcasted_iota(jnp.int32, (TILE, TILE), 0) >= lax.broadcasted_iota(
                jnp.int32, (TILE, TILE), 1
            )
            parts.append((jnp.where(keep, scores, -1e30), vl_ref[pl.ds(full, TILE), :]))
            row_max = functools.reduce(
                jnp.maximum, [jnp.max(s, axis=1, keepdims=True) for s, unused in parts]
            )
            mixed = None
            for s, value in parts:
                exponent = jnp.exp(s - row_max)
                part_total = jnp.sum(exponent, axis=1, keepdims=True)
                part_mixed = dot(exponent.astype(BF16), value)
                mixed = part_mixed if mixed is None else mixed + part_mixed
                total = part_total if s is parts[0][0] else total + part_total
            result = (mixed / total).astype(BF16)
            log_row = jnp.transpose(
                jnp.broadcast_to(row_max + jnp.log(total), (TILE, LANES))
            )[0:1, :]

            @pl.when(head == 0)
            def _():
                out_ref[here, :] = result
                lse_ref[0, 0:1, here] = log_row

            @pl.when(head == 1)
            def _():
                out_ref[here, :] = jnp.where(mask, result, out_ref[here, :])
                lse_ref[0, 1:2, here] = log_row

    @pl.when(flag_ref[0] == 0)
    def _():
        run(False)

    @pl.when(flag_ref[0] != 0)
    def _():
        run(True)


def attend(flag, queries, key_own, value_own, key_far, value_far, chunk):
    row_count, width = queries.shape
    rows = row_count // CHUNKS
    pairs = width // LANES

    def spec(size, block):
        return pl.BlockSpec((size, LANES), lambda g: (block, g // 2))

    work = rows * (row_count + row_count // 2) * 2 * pairs
    return pl.pallas_call(
        functools.partial(attend_kernel, chunk),
        out_shape=(
            jax.ShapeDtypeStruct((rows, width), BF16),
            jax.ShapeDtypeStruct((pairs, 2, rows), F32),
        ),
        grid=(2 * pairs,),
        in_specs=[
            pl.BlockSpec(memory_space=pltpu.SMEM),
            spec(rows, chunk),
            spec(row_count, 0),
            spec(row_count, 0),
            spec(row_count, 0),
            spec(row_count, 0),
        ],
        out_specs=(spec(rows, 0), pl.BlockSpec((1, 2, rows), lambda g: (g // 2, 0, 0))),
        cost_estimate=pl.CostEstimate(
            flops=4 * HEAD_DIM * work * 4, bytes_accessed=12 * width * row_count, transcendentals=work
        ),
        name="attend",
    )(flag, queries, key_own, value_own, key_far, value_far)


def attend_back_kernel(
    flag_ref, q_ref, kl_ref, vl_ref, kr_ref, vr_ref, out_ref, grad_ref, lse_ref,
    dq_ref, dkl_ref, dvl_ref, dkr_ref, dvr_ref, key_acc, value_acc, query_acc,
):
    head = pl.program_id(0) % 2
    row_count = q_ref.shape[0]

    @pl.when(head == 0)
    def _():
        key_acc[...] = jnp.zeros_like(key_acc)
        value_acc[...] = jnp.zeros_like(value_acc)

    def run(remote):
        own_t = jnp.transpose(kl_ref[...])
        far_t = jnp.transpose(kr_ref[...]) if remote else None
        for t in range(row_count // TILE):
            here = pl.ds(t * TILE, TILE)
            mask = head_lanes(head, (TILE, LANES))
            query = jnp.where(mask, q_ref[here, :] * BF16(SCALING), BF16(0))
            grad = jnp.where(mask, grad_ref[here, :], BF16(0))
            both = jnp.transpose(grad.astype(F32) * out_ref[here, :].astype(F32))
            correction = jnp.sum(both, axis=0, keepdims=True)
            lse = lse_ref[0, pl.ds(head, 1), here]
            full = t * TILE
            parts = []
            if remote:
                parts.append((kr_ref[...], vr_ref[...], far_t, row_count, row_count, False))
            if full:
                before = pl.ds(0, full)
                parts.append((kl_ref[before, :], vl_ref[before, :], own_t[:, :full], 0, full, False))
            parts.append(
                (kl_ref[here, :], vl_ref[here, :], own_t[:, full : full + TILE], full, TILE, True)
            )
            query_t = None
            for key, value, key_t, offset, size, diagonal in parts:
                scores = dot(key, query, NT)
                if diagonal:
                    keep = lax.broadcasted_iota(
                        jnp.int32, (TILE, TILE), 1
                    ) >= lax.broadcasted_iota(jnp.int32, (TILE, TILE), 0)
                    scores = jnp.where(keep, scores, -1e30)
                prob = jnp.exp(scores - lse)
                prob_grad = dot(value, grad, NT)
                score_grad = (prob * (prob_grad - correction)).astype(BF16)
                value_acc[pl.ds(offset, size), :] += dot(prob.astype(BF16), grad)
                key_acc[pl.ds(offset, size), :] += dot(score_grad, query)
                part = dot(key_t, score_grad)
                query_t = part if query_t is None else query_t + part
            query_grad = jnp.transpose(query_t) * SCALING

            @pl.when(head == 0)
            def _():
                query_acc[here, :] = query_grad

            @pl.when(head == 1)
            def _():
                dq_ref[here, :] = jnp.where(mask, query_grad, query_acc[here, :]).astype(BF16)

    @pl.when(flag_ref[0] == 0)
    def _():
        run(False)

    @pl.when(flag_ref[0] != 0)
    def _():
        run(True)

    @pl.when(head == 1)
    def _():
        own, far = pl.ds(0, row_count), pl.ds(row_count, row_count)
        dkl_ref[...] = key_acc[own, :].astype(BF16)
        dvl_ref[...] = value_acc[own, :].astype(BF16)
        dkr_ref[...] = key_acc[far, :].astype(BF16)
        dvr_ref[...] = value_acc[far, :].astype(BF16)


def attend_back(flag, queries, key_own, value_own, key_far, value_far, mixed, grad, lse):
    row_count, width = queries.shape
    pairs = width // LANES
    spec = pl.BlockSpec((row_count, LANES), lambda g: (0, g // 2))
    shape = jax.ShapeDtypeStruct((row_count, width), BF16)
    work = row_count * (row_count + row_count // 2) * 2 * pairs
    return pl.pallas_call(
        attend_back_kernel,
        out_shape=(shape,) * 5,
        grid=(2 * pairs,),
        in_specs=[pl.BlockSpec(memory_space=pltpu.SMEM)]
        + [spec] * 7
        + [pl.BlockSpec((1, 2, row_count), lambda g: (g // 2, 0, 0))],
        out_specs=(spec,) * 5,
        scratch_shapes=[pltpu.VMEM((2 * row_count, LANES), F32)] * 2
        + [pltpu.VMEM((row_count, LANES), F32)],
        cost_estimate=pl.CostEstimate(
            flops=10 * HEAD_DIM * work * 3, bytes_accessed=24 * width * row_count, transcendentals=work
        ),
        name="attend_back",
    )(flag, queries, key_own, value_own, key_far, value_far, mixed, grad, lse)


def cross_kernel(q_ref, key_ref, value_ref, out_ref):
    for pair in range(q_ref.shape[1] // LANES):
        lanes = pl.ds(pair * LANES, LANES)
        query, key, value = q_ref[:, lanes], key_ref[:, lanes], value_ref[:, lanes]
        mixed = None
        for head in range(2):
            mask = head_lanes(head, key.shape)
            scores = dot(jnp.where(mask, key * BF16(SCALING), BF16(0)), query, NT)
            exponent = jnp.exp(scores - jnp.max(scores, axis=0, keepdims=True))
            prob = exponent / jnp.sum(exponent, axis=0, keepdims=True)
            part = dot(prob.astype(BF16), jnp.where(mask, value, BF16(0)), TN)
            mixed = part if mixed is None else mixed + part
        out_ref[:, lanes] = mixed.astype(BF16)


def cross_attend(queries, key_text, value_text):
    rows, width = queries.shape
    work = rows * key_text.shape[0] * width // HEAD_DIM
    return pl.pallas_call(
        cross_kernel,
        out_shape=jax.ShapeDtypeStruct((rows, width), BF16),
        cost_estimate=pl.CostEstimate(
            flops=16 * HEAD_DIM * work, bytes_accessed=4 * width * rows, transcendentals=work
        ),
        name="cross_attend",
    )(queries, key_text, value_text)


def cross_back_kernel(q_ref, key_ref, value_ref, grad_ref, dq_ref, dkey_ref, dvalue_ref):
    for pair in range(q_ref.shape[1] // LANES):
        lanes = pl.ds(pair * LANES, LANES)
        query, key, value = q_ref[:, lanes], key_ref[:, lanes], value_ref[:, lanes]
        grad = grad_ref[:, lanes]
        query_grad, key_grad, value_grad = None, None, None
        for head in range(2):
            mask = head_lanes(head, key.shape)
            key_head = jnp.where(mask, key * BF16(SCALING), BF16(0))
            scores = dot(key_head, query, NT)
            exponent = jnp.exp(scores - jnp.max(scores, axis=0, keepdims=True))
            prob = exponent / jnp.sum(exponent, axis=0, keepdims=True)
            prob_grad = dot(jnp.where(mask, value, BF16(0)), grad, NT)
            correction = jnp.sum(prob * prob_grad, axis=0, keepdims=True)
            score_grad = (prob * (prob_grad - correction)).astype(BF16)
            part = dot(score_grad, key_head, TN)
            key_part = jnp.where(mask, dot(score_grad, query), 0.0)
            value_part = jnp.where(mask, dot(prob.astype(BF16), grad), 0.0)
            if head == 0:
                query_grad, key_grad, value_grad = part, key_part, value_part
            else:
                query_grad, key_grad, value_grad = (
                    query_grad + part,
                    key_grad + key_part,
                    value_grad + value_part,
                )
        dq_ref[:, lanes] = query_grad.astype(BF16)
        dkey_ref[:, lanes] = key_grad * SCALING
        dvalue_ref[:, lanes] = value_grad


def cross_attend_back(queries, key_text, value_text, grad):
    rows, width = queries.shape
    texts = key_text.shape[0]
    work = rows * texts * width // HEAD_DIM
    text_shape = jax.ShapeDtypeStruct((texts, width), F32)
    return pl.pallas_call(
        cross_back_kernel,
        out_shape=(jax.ShapeDtypeStruct((rows, width), BF16), text_shape, text_shape),
        cost_estimate=pl.CostEstimate(
            flops=40 * HEAD_DIM * work, bytes_accessed=6 * width * rows, transcendentals=work
        ),
        name="cross_attend_back",
    )(queries, key_text, value_text, grad)


def moments(values):
    centered = values - jnp.mean(values, axis=-1, keepdims=True)
    scale = lax.rsqrt(jnp.mean(centered * centered, axis=-1, keepdims=True) + EPSILON)
    return centered * scale, scale


def layer_norm(values, gain, bias):
    unit, unused = moments(values)
    return (unit * gain + bias).astype(BF16)


def norm_back(values, gain, grad):
    unit, scale = moments(values)
    inner = grad * gain
    shift = jnp.mean(inner, axis=-1, keepdims=True)
    slope = jnp.mean(inner * unit, axis=-1, keepdims=True)
    value_grad = scale * (inner - shift - unit * slope)
    return value_grad, jnp.sum(grad * unit, axis=0), jnp.sum(grad, axis=0)


def gray(place):
    return place ^ (place >> 1)


def cut(values, start, size, axis=0):
    return lax.dynamic_slice_in_dim(values, start, size, axis)


def put(whole, part, start, axis=0):
    return lax.dynamic_update_slice_in_dim(whole, part, start, axis)


class Plan:
    def __init__(self, mesh):
        self.sizes = dict(mesh.shape)
        self.shards = self.sizes["shard"]
        assert self.sizes["tp"] == 4 and self.sizes["ctx"] == 2

    def swap(self, values, axis, bit):
        return lax.ppermute(values, axis, [(i, i ^ bit) for i in range(self.sizes[axis])])

    def near(self, values):
        return self.swap(values, "tp", 1)

    def across(self, values):
        return self.swap(values, "tp", 2)

    def beside(self, values):
        return self.swap(values, "ctx", 1)

    def onward(self, values):
        n = self.shards
        return lax.ppermute(values, "shard", [(gray(p), gray((p + 1) % n)) for p in range(n)])

    def place(self, back):
        here = gray(lax.axis_index("shard"))
        return gray((here + self.shards - back) % self.shards)

    def sum_over(self, values, axis):
        bit = 1
        while bit < self.sizes[axis]:
            values = values + self.swap(values, axis, bit)
            bit *= 2
        return values

    def gather_small(self, values, axis):
        n = self.shards
        size = values.shape[axis]
        here = lax.axis_index("shard")
        shape = list(values.shape)
        shape[axis] = size * n
        whole = put(jnp.zeros(shape, values.dtype), values, here * size, axis)
        bit = 1
        held = [(here, values)]
        while bit < n:
            stacked = jnp.stack([block for unused, block in held])
            came = self.swap(stacked, "shard", bit)
            fresh = [(idx ^ bit, came[i]) for i, (idx, unused) in enumerate(held)]
            for idx, block in fresh:
                whole = put(whole, block, idx * size, axis)
            held = held + fresh
            bit *= 2
        return whole

    def gather_weights(self, weights, axes):
        if self.shards != 4:
            return [
                lax.all_gather(w, "shard", axis=axis, tiled=True) for w, axis in zip(weights, axes)
            ]
        side = lax.axis_index("ctx")
        here = lax.axis_index("shard")
        halves = [w.shape[0] // 2 for w in weights]
        sent = [cut(w, side * half, half) for w, half in zip(weights, halves)]
        same = len({s.shape for s in sent}) == 1
        packed = jnp.stack(sent) if same else None
        assert same
        wholes = []
        for w, axis in zip(weights, axes):
            shape = list(w.shape)
            shape[axis] *= self.shards
            wholes.append(put(jnp.zeros(shape, w.dtype), w, here * w.shape[axis], axis))
        for step in range(1, self.shards):
            packed = self.onward(packed)
            other = self.beside(packed)
            source = self.place(step)
            for i, (w, axis, half) in enumerate(zip(weights, axes, halves)):
                for block, which in ((packed[i], side), (other[i], 1 - side)):
                    start = [which * half, 0]
                    start[axis] = start[axis] + source * w.shape[axis]
                    wholes[i] = lax.dynamic_update_slice(wholes[i], block, start)
        return wholes

    def ring_sum(self, block_of):
        travels = block_of(self.place(1))
        for step in range(2, self.shards + 1):
            came = self.onward(travels)
            total = came.astype(F32) + block_of(self.place(step % self.shards)).astype(F32)
            travels = total.astype(BF16)
        return total

    def reduce_grad(self, partial, axis, beside_first):
        n = self.shards
        size = partial.shape[axis] // n
        partial = partial.astype(BF16)
        if n != 4:
            mine = lax.psum_scatter(partial, "shard", scatter_dimension=axis, tiled=True)
            mine = mine.astype(BF16)
            return mine.astype(F32) + self.beside(mine).astype(F32)
        if not beside_first:
            mine = self.ring_sum(lambda j: cut(partial, j * size, size, axis)).astype(BF16)
            return mine.astype(F32) + self.beside(mine).astype(F32)
        side = lax.axis_index("ctx")
        if axis == 0:
            half = size // 2
            split = partial.reshape(n, 2, half, partial.shape[1])
            away = cut(split, 1 - side, 1, 1)[:, 0]
            keep = cut(split, side, 1, 1)[:, 0]
            joined = (keep.astype(F32) + self.beside(away).astype(F32)).astype(BF16)
            mine = self.ring_sum(lambda j: cut(joined, j, 1)[0])
        else:
            half = partial.shape[0] // 2
            away = cut(partial, (1 - side) * half, half)
            keep = cut(partial, side * half, half)
            joined = (keep.astype(F32) + self.beside(away).astype(F32)).astype(BF16)
            mine = self.ring_sum(lambda j: cut(joined, j * size, size, 1))
        mine = mine.astype(BF16)
        other = self.beside(mine)
        whole = jnp.zeros((2 * half, mine.shape[1]), F32)
        whole = put(whole, mine.astype(F32), side * half)
        return put(whole, other.astype(F32), (1 - side) * half)


def on_device(
    plan,
    inputs,
    text_states,
    query_self,
    key_self,
    value_self,
    output_self,
    query_cross,
    key_cross,
    value_cross,
    output_cross,
    up_weight,
    down_weight,
    gain_self,
    bias_self,
    gain_cross,
    bias_cross,
    gain_feed,
    bias_feed,
    cotangent,
):
    core = lax.axis_index("tp") % 2
    side = lax.axis_index("ctx")
    shard = lax.axis_index("shard")
    flag = jnp.full((1,), side, jnp.int32)
    stream = inputs[0]
    upstream = cotangent[0]
    row_count = stream.shape[0]
    rows = row_count // CHUNKS
    half = rows // 2
    own_width = query_self.shape[0]

    def mine_of(values, chunk):
        return cut(values, chunk * rows + core * half, half)

    def other_of(values, chunk):
        return cut(values, chunk * rows + (1 - core) * half, half)

    def relative(values, chunk):
        return jnp.concatenate([mine_of(values, chunk), other_of(values, chunk)])

    def total_of(mine, other):
        joined = (mine + plan.near(other.astype(BF16)).astype(F32)).astype(BF16)
        return joined.astype(F32) + plan.across(joined).astype(F32)

    def total_rows(values, weight, dims=NN):
        return total_of(dot(values[:half], weight, dims), dot(values[half:], weight, dims))

    def whole_rows(mine):
        return jnp.concatenate([mine, plan.near(mine)])

    def absolute(pieces):
        whole = jnp.zeros((row_count, pieces[0][0].shape[1]), pieces[0][0].dtype)
        for chunk, (mine, other) in enumerate(pieces):
            whole = put(whole, mine, chunk * rows + core * half)
            whole = put(whole, other, chunk * rows + (1 - core) * half)
        return whole

    vectors = jnp.stack([gain_self, bias_self, gain_cross, bias_cross, gain_feed, bias_feed])
    vectors = plan.gather_small(vectors, 1).astype(F32)
    self_gain, self_bias, cross_gain, cross_bias, feed_gain, feed_bias = (
        vectors[i] for i in range(6)
    )
    wq, wk, wv = plan.gather_weights([query_self, key_self, value_self], [0, 0, 0])
    wo, wcq, wco = plan.gather_weights([output_self, query_cross, output_cross], [1, 0, 1])
    (w_up,) = plan.gather_weights([up_weight], [0])
    (w_down,) = plan.gather_weights([down_weight], [1])

    text_own = cut(text_states, shard * own_width, own_width, 1)
    text_part = jnp.concatenate([dot(text_own, key_cross), dot(text_own, value_cross)], axis=1)
    text_both = plan.sum_over(text_part, "shard").astype(BF16)
    head_width = key_cross.shape[1]
    key_text, value_text = text_both[:, :head_width], text_both[:, head_width:]

    normed_self = layer_norm(stream.astype(F32), self_gain, self_bias)
    key_own = dot(normed_self, wk).astype(BF16)
    value_own = dot(normed_self, wv).astype(BF16)
    key_far, value_far = plan.beside(key_own), plan.beside(value_own)
    queries = dot(normed_self, wq).astype(BF16)

    chunks = range(CHUNKS)
    mixed, lse, after_self, normed_cross, cross_rows = [], [], [], [], []
    crossed, after_cross, normed_feed, hidden_pre, hidden = [], [], [], [], []
    layer_pieces = []
    grad_feed = [relative(upstream, c) for c in chunks]
    for c in chunks:
        out, log_total = attend(flag, queries, key_own, value_own, key_far, value_far, c)
        lse.append(log_total)
        mixed.append(out)
        other = dot(cut(out, (1 - core) * half, half), wo)
        mine = dot(cut(out, core * half, half), wo)
        after_self.append(mine_of(stream, c).astype(F32) + total_of(mine, other))
        normed_cross.append(whole_rows(layer_norm(after_self[c], cross_gain, cross_bias)))
        cross_rows.append(dot(normed_cross[c], wcq).astype(BF16))
        crossed.append(cross_attend(cross_rows[c], key_text, value_text))
        after_cross.append(after_self[c] + total_rows(crossed[c], wco))
        normed_feed.append(whole_rows(layer_norm(after_cross[c], feed_gain, feed_bias)))
        hidden_pre.append(dot(normed_feed[c], w_up))
        hidden.append(jax.nn.gelu(hidden_pre[c], approximate=False).astype(BF16))
        layer_mine = (after_cross[c] + total_rows(hidden[c], w_down)).astype(BF16)
        layer_pieces.append((layer_mine, plan.near(layer_mine)))
    layer_out = absolute(layer_pieces)

    hidden_grad = [dot(grad_feed[c], w_down, NT) for c in chunks]
    down_part = dot(jnp.concatenate(hidden), jnp.concatenate(grad_feed), TN)
    down_grad = plan.reduce_grad(down_part, 1, False)
    pre_grad, cross_stream, grad_cross = [], [], []
    vector_parts = {"feed": [], "cross": [], "self": []}
    for c in chunks:
        unused, pull = jax.vjp(functools.partial(jax.nn.gelu, approximate=False), hidden_pre[c])
        pre_grad.append(pull(hidden_grad[c])[0].astype(BF16))
        summed = total_rows(pre_grad[c], w_up, NT)
        feed_in, gain_part, bias_part = norm_back(after_cross[c], feed_gain, summed)
        vector_parts["feed"].append(jnp.stack([gain_part, bias_part]))
        cross_stream.append(mine_of(upstream, c).astype(F32) + feed_in)
        grad_cross.append(whole_rows(cross_stream[c].astype(BF16)))
    up_part = dot(jnp.concatenate(normed_feed), jnp.concatenate(pre_grad), TN)
    up_grad = plan.reduce_grad(up_part, 0, True)

    crossq_low, text_keys, text_values, grad_self, self_stream = [], [], [], [], []
    for c in chunks:
        crossed_grad = dot(grad_cross[c], wco, NT).astype(BF16)
        crossq, text_key, text_value = cross_attend_back(
            cross_rows[c], key_text, value_text, crossed_grad
        )
        crossq_low.append(crossq)
        text_keys.append(text_key)
        text_values.append(text_value)
        summed = total_rows(crossq, wcq, NT)
        cross_in, gain_part, bias_part = norm_back(after_self[c], cross_gain, summed)
        vector_parts["cross"].append(jnp.stack([gain_part, bias_part]))
        self_stream.append(cross_stream[c] + cross_in)
        grad_self.append(whole_rows(self_stream[c].astype(BF16)))
    crossed_all = jnp.concatenate(crossed)
    outputcross_grad = plan.reduce_grad(dot(crossed_all, jnp.concatenate(grad_cross), TN), 1, True)
    querycross_grad = plan.reduce_grad(
        dot(jnp.concatenate(normed_cross), jnp.concatenate(crossq_low), TN), 0, True
    )
    text_sum = jnp.concatenate([sum(text_keys), sum(text_values)], axis=1)
    text_sum = plan.sum_over(plan.sum_over(text_sum, "ctx"), "shard")
    text_key, text_value = text_sum[:, :head_width], text_sum[:, head_width:]
    text_float = text_own.astype(F32)
    keycross_grad = jnp.dot(text_float.T, text_key, precision=HIGH)
    valuecross_grad = jnp.dot(text_float.T, text_value, precision=HIGH)
    text_grad = jnp.dot(text_key, key_cross.astype(F32).T, precision=HIGH) + jnp.dot(
        text_value, value_cross.astype(F32).T, precision=HIGH
    )
    text_grad = plan.gather_small(plan.sum_over(text_grad, "tp"), 1)

    attended_pieces = []
    for c in chunks:
        attended_grad = dot(grad_self[c], wo, NT).astype(BF16)
        attended_pieces.append((attended_grad[:half], attended_grad[half:]))
    mixed_all = jnp.concatenate(mixed)
    grad_self_all = absolute([(g[:half], g[half:]) for g in grad_self])
    outputself_grad = plan.reduce_grad(dot(mixed_all, grad_self_all, TN), 1, True)
    query_low, key_low, value_low, key_back, value_back = attend_back(
        flag,
        queries,
        key_own,
        value_own,
        key_far,
        value_far,
        mixed_all,
        absolute(attended_pieces),
        jnp.concatenate(lse, axis=2),
    )
    wide = plan.sizes["ctx"]
    home = [(i, i - 1) for i in range(1, wide)]
    key_low = (key_low.astype(F32) + lax.ppermute(key_back, "ctx", home).astype(F32)).astype(BF16)
    value_low = (
        value_low.astype(F32) + lax.ppermute(value_back, "ctx", home).astype(F32)
    ).astype(BF16)
    input_pieces = []
    for c in chunks:

        def part(pick):
            return (
                dot(pick(query_low, c), wq, NT)
                + dot(pick(key_low, c), wk, NT)
                + dot(pick(value_low, c), wv, NT)
            )

        summed = total_of(part(mine_of), part(other_of))
        self_in, gain_part, bias_part = norm_back(mine_of(stream, c).astype(F32), self_gain, summed)
        vector_parts["self"].append(jnp.stack([gain_part, bias_part]))
        input_mine = (self_stream[c] + self_in).astype(BF16)
        input_pieces.append((input_mine, plan.near(input_mine)))
    input_grad = absolute(input_pieces)
    queryself_grad = plan.reduce_grad(dot(normed_self, query_low, TN), 0, True)
    keyself_grad = plan.reduce_grad(dot(normed_self, key_low, TN), 0, True)
    valueself_grad = plan.reduce_grad(dot(normed_self, value_low, TN), 0, True)

    def vector_grads(parts):
        total = plan.near(parts) + parts
        total = plan.sum_over(plan.sum_over(total, "ctx"), "shard")
        return cut(total, shard * own_width, own_width, 1)

    early = vector_grads(
        jnp.concatenate([sum(vector_parts["cross"]), sum(vector_parts["feed"])])
    )
    late = vector_grads(sum(vector_parts["self"]))
    return (
        layer_out[None],
        input_grad[None],
        text_grad,
        queryself_grad,
        keyself_grad,
        valueself_grad,
        outputself_grad,
        querycross_grad,
        keycross_grad,
        valuecross_grad,
        outputcross_grad,
        up_grad,
        down_grad,
        late[0],
        late[1],
        early[0],
        early[1],
        early[2],
        early[3],
    )


def solution(mesh):
    placed = (
        P("shard", "ctx", None),
        P(),
        P("shard", "tp"),
        P("shard", "tp"),
        P("shard", "tp"),
        P("tp", "shard"),
        P("shard", "tp"),
        P("shard", "tp"),
        P("shard", "tp"),
        P("tp", "shard"),
        P("shard", "tp"),
        P("tp", "shard"),
        P("shard"),
        P("shard"),
        P("shard"),
        P("shard"),
        P("shard"),
        P("shard"),
        P("shard", "ctx", None),
    )
    return jax.shard_map(
        functools.partial(on_device, Plan(mesh)),
        mesh=mesh,
        in_specs=placed,
        out_specs=(
            P("shard", "ctx", None),
            P("shard", "ctx", None),
            P(),
            P("shard", "tp"),
            P("shard", "tp"),
            P("shard", "tp"),
            P("tp", "shard"),
            P("shard", "tp"),
            P("shard", "tp"),
            P("shard", "tp"),
            P("tp", "shard"),
            P("shard", "tp"),
            P("tp", "shard"),
            P("shard"),
            P("shard"),
            P("shard"),
            P("shard"),
            P("shard"),
            P("shard"),
        ),
        check_vma=False,
    )
```
